32 devices in a mesh: sta: 16 (over z, x, core), tpl: 2 (over y).
Axes of the slice: x: 2, y: 2, z: 4, core: 2. Of those that a mesh axis runs over, the one named last changes fastest.
Arguments:
- waveform: bfloat16 [16, 3, 4279], P('sta'), may hold values from -150 to 150
- templates: bfloat16 [128, 16, 1536], P('tpl', 'sta'), may hold values from -6 to 6
- lags: int32 [128, 16], P('tpl', 'sta'), may hold values from 0 to 3000
- present: int32 [128, 16], P('tpl', 'sta'), may hold values 0 or 1
Outputs:
- score: float32 [768, 128], P('sta', 'tpl')
- scale_mad: float32 [128], P('tpl')
- peak: float32 [768], P('sta')
The draws below stay inside these ranges and needn't reach their ends.
All inputs are finite; a program needn't handle non-finite values. No bound on the sum of `present` on one device may be relied on, other than what follows from the above.
Results may differ from the reference program's by a relative error of at most 0.0003.
Values may be sent and summed in bfloat16 or wider, within the bound.
A program may use at most 64 MiB of HBM per device.

```python
import jax
import jax.numpy as jnp
from jax import lax

LEN = 512
CHANS = 3
LAG = 3000
BINS = 1024
STATIONS = 16
TEMPLATES = 128
TOUT = 768
SAMPLES = 4279


def draw_waveform(key, part):
    key_noise = jax.random.fold_in(key, 11)
    key_scale = jax.random.fold_in(key, 12)
    timeline = jnp.arange(SAMPLES, dtype=jnp.float32) / SAMPLES
    envelope = jnp.exp(jnp.log(3.0) * timeline)
    noise = jnp.clip(jax.random.normal(key_noise, (STATIONS, 3, SAMPLES), jnp.float32), -5.0, 5.0)
    scales = jnp.exp(jax.random.uniform(key_scale, (STATIONS, 1, 1), jnp.float32, 0.0, jnp.log(10.0)))
    return (noise * scales * envelope).astype(jnp.bfloat16)


def touch_ends(drawn, own_key, smallest, top_value):
    longest = drawn.shape.index(max(drawn.shape))
    spots = []
    for shift in (0, 1):
        where = [jax.random.randint(jax.random.fold_in(own_key, axis), (), 0, length) for axis, length in enumerate(drawn.shape)]
        where[longest] = (where[longest] + shift) % drawn.shape[longest]
        spots.append(tuple(where))
    return drawn.at[spots[0]].set(smallest).at[spots[1]].set(top_value)


def shard_levels(own_key, extent, shards, least, high):
    loudness, own = 1.0, jax.random.fold_in(own_key, 6)
    for axis_at, blocks in shards:
        draws = jnp.exp(jax.random.uniform(jax.random.fold_in(own, axis_at), (blocks,), jnp.float32, least / len(shards), high / len(shards)))
        loudness = loudness * jnp.repeat(draws, extent[axis_at] // blocks).reshape([-1 if axis == axis_at else 1 for axis in range(len(extent))])
    return loudness


def normal_values(own_key, extent, scale, most, pieces=(), held_as=jnp.bfloat16):
    values = scale * jax.random.normal(own_key, extent, jnp.float32)
    if pieces:
        values = values * shard_levels(own_key, extent, pieces, -0.22, 0.18)
    return jnp.clip(values, -most, most).astype(held_as)


def setup_inputs(seed: int = 0) -> dict:
    streams_of = jax.random.split(jax.random.key(seed), 5)
    waveform = draw_waveform(jax.random.fold_in(streams_of[4], 71), 0)
    templates = normal_values(streams_of[1], (TEMPLATES, STATIONS, CHANS * LEN), 1.0, 6.0, ((0, 2), (1, 16)))
    lags = touch_ends(jax.random.randint(streams_of[2], (TEMPLATES, STATIONS), 0, LAG + 1), jax.random.fold_in(streams_of[2], 1), 0, LAG).astype(jnp.int32)
    present = touch_ends((jax.random.randint(streams_of[3], (TEMPLATES, STATIONS), 0, 4) < 3).astype(jnp.int32), jax.random.fold_in(streams_of[3], 1), 0, 1)
    return dict(waveform=waveform, templates=templates, lags=lags, present=present)


def toeplitz_rows(record, length, columns):
    count = record.shape[1]
    chans = record.shape[0]
    tiled = jnp.broadcast_to(record[:, None, :], (chans, length + 1, count))
    tiled = tiled.reshape(chans, (length + 1) * count)[:, :length * (count + 1)]
    tiled = tiled.reshape(chans, length, count + 1)[:, :, :columns]
    return tiled.reshape(chans * length, columns)

def shift_rows(block, offsets, count):
    return jax.vmap(lambda row, offset: lax.dynamic_slice_in_dim(row, offset, count))(block, offsets.astype(jnp.int32))

def hat_counts(values, nbins):
    width = 512.0 / nbins
    ncols = values.shape[1]
    position = jnp.clip(jnp.abs(values) / width - 0.5, 0.0, nbins - 1.0)
    lower = jnp.minimum(jnp.floor(position), nbins - 2.0)
    weight = position - lower
    index = lower.astype(jnp.int32) + nbins * jnp.arange(ncols, dtype=jnp.int32)[None, :]
    flat_index = index.reshape(-1)
    flat_weight = weight.reshape(-1)
    counts = jax.ops.segment_sum(1.0 - flat_weight, flat_index, num_segments=ncols * nbins)
    counts = counts + jax.ops.segment_sum(flat_weight, flat_index + 1, num_segments=ncols * nbins)
    return counts.reshape(ncols, nbins)

def median_abs(counts, halfway):
    width = 512.0 / counts.shape[1]
    running = jnp.cumsum(counts, axis=1)
    earlier = running - counts
    share = jnp.clip((halfway - earlier) / jnp.maximum(counts, 1.0), 0.0, 1.0)
    return width * lax.optimization_barrier(jnp.sum(share, axis=1))

def reference(waveform, templates, lags, present):
    total = TOUT
    span = TOUT + LAG
    tnorm = jnp.sqrt(lax.optimization_barrier(jnp.sum(templates.astype(jnp.float32) ** 2, axis=2)) + 1e-06)

    def station(stack, items):
        record, pattern, offsets, member, scaling = items
        columns = toeplitz_rows(record, LEN, span)
        corr = jnp.dot(pattern, columns, preferred_element_type=jnp.float32) / scaling[:, None]
        moved = shift_rows(corr, offsets, total) * member[:, None].astype(jnp.float32)
        return (stack + moved, None)
    start = jnp.zeros((templates.shape[0], total), jnp.float32)
    stack, unused = lax.scan(station, start, (waveform, jnp.swapaxes(templates, 0, 1), lags.T, present.T, tnorm.T))
    stack = stack.T
    counts = hat_counts(stack, BINS)
    median = median_abs(counts, 0.5 * total)
    scale_mad = 1.4826 * median
    score = stack / scale_mad[None, :]
    peak = lax.optimization_barrier(jnp.max(score, axis=1))
    return (score, scale_mad, peak)
```

```python
import functools

import jax
import jax.numpy as jnp
from jax import lax
from jax.experimental import pallas as pl
from jax.experimental.pallas import tpu as pltpu
from jax.sharding import PartitionSpec as P

LEN = 512
LAG = 3000
BINS = 1024
TOUT_DEV = 48
LANES = 128
MESH = pl.DeviceIdType.MESH


def ceil_to(value, step):
    return -(-value // step) * step


def correlate_kernel(blocks, stride, lags_ref, wave_ref, pattern_ref, present_ref, moved_ref, record, hankel, corr):
    chans, samples = wave_ref.shape
    rows = pattern_ref.shape[0]
    padded = record.shape[1]
    span = hankel.shape[2]
    width = padded - LANES
    record[...] = jnp.zeros_like(record)
    record[:, :samples] = wave_ref[...].astype(jnp.float32)
    row = lax.broadcasted_iota(jnp.int32, (8, padded), 0)
    for c in range(chans):
        base = jnp.broadcast_to(record[c : c + 1, :], (8, padded))
        for bit in (1, 2, 4):
            base = jnp.where((row & bit) != 0, pltpu.roll(base, padded - bit, 1), base)
        for g in range(LANES // 16):
            low = pltpu.roll(base, padded - 16 * g, 1) if g else base
            high = pltpu.roll(base, padded - 16 * g - 8, 1)
            both = jnp.concatenate([low[:, :span], high[:, :span]], axis=0)
            hankel[c, 16 * g : 16 * g + 16, :] = both.astype(jnp.bfloat16)
    pattern = pattern_ref[...]
    wide = pattern.astype(jnp.float32)
    scaling = jnp.sqrt(jnp.sum(wide * wide, axis=1, keepdims=True) + 1e-06)
    factor = present_ref[...].astype(jnp.float32) / scaling
    for b in range(blocks):
        parts = []
        for c in range(chans):
            for q in range(LEN // LANES):
                begin = 2 * LANES * b + LANES * q
                parts.append(hankel[c, :, begin : begin + 2 * LANES])
        columns = jnp.concatenate(parts, axis=0)
        result = jnp.dot(pattern, columns, preferred_element_type=jnp.float32) * factor
        corr[pl.ds(2 * b, rows, stride=stride), :] = result[:, :LANES]
        corr[pl.ds(2 * b + 1, rows, stride=stride), :] = result[:, LANES:]
    count = moved_ref.shape[0] // rows
    lane = lax.broadcasted_iota(jnp.int32, (count, LANES), 1)
    for t in range(rows):
        lag = lags_ref[t]
        begin = t * stride + (lag >> 7)
        rest = lag & (LANES - 1)
        near = corr[pl.ds(begin, count), :]
        after = corr[pl.ds(begin + 1, count), :]
        joined = jnp.where(lane >= rest, near, after)
        moved_ref[t * count : (t + 1) * count, :] = pltpu.roll(joined, (LANES - rest) & (LANES - 1), 1)


def correlate(wave, pattern, lags, present, total):
    chans, samples = wave.shape
    rows = pattern.shape[0]
    blocks = -(-(total + LAG) // (2 * LANES))
    span = 2 * LANES * blocks + LEN - LANES
    padded = span + LANES
    count = total // LANES
    stride = max(2 * blocks, LAG // LANES + count + 2) | 1
    return pl.pallas_call(
        functools.partial(correlate_kernel, blocks, stride),
        out_shape=jax.ShapeDtypeStruct((rows * count, LANES), jnp.float32),
        in_specs=[pl.BlockSpec(memory_space=pltpu.SMEM)] + [pl.BlockSpec(memory_space=pltpu.VMEM)] * 3,
        out_specs=pl.BlockSpec(memory_space=pltpu.VMEM),
        scratch_shapes=[
            pltpu.VMEM((chans, padded), jnp.float32),
            pltpu.VMEM((chans, LANES, span), jnp.bfloat16),
            pltpu.VMEM((rows * stride, LANES), jnp.float32),
        ],
    )(lags, wave, pattern, present)


def deviation_scale(stack, groups, total):
    width = 512.0 / BINS
    count = stack.shape[0] // groups
    position = jnp.clip(jnp.abs(stack) / width - 0.5, 0.0, BINS - 1.0)
    lower = jnp.minimum(jnp.floor(position), BINS - 2.0)
    coarse = jnp.floor(lower * 0.125)
    fine = position - 8.0 * coarse
    sub = lax.broadcasted_iota(jnp.int32, (LANES, LANES), 0).astype(jnp.float32)
    few = lax.broadcasted_iota(jnp.int32, (16, LANES), 0).astype(jnp.float32)
    tables = []
    for t in range(groups):
        hots, weights = [], []
        for a in range(count):
            r = t * count + a
            hots.append((coarse[r : r + 1, :] == sub).astype(jnp.float32).astype(jnp.bfloat16))
            hat = jnp.maximum(1.0 - jnp.abs(fine[r : r + 1, :] - few), 0.0)
            first = hat.astype(jnp.bfloat16)
            left = hat - first.astype(jnp.float32)
            second = left.astype(jnp.bfloat16)
            third = (left - second.astype(jnp.float32)).astype(jnp.bfloat16)
            weights.append(jnp.concatenate([first, second, third], axis=0))
        hot = jnp.concatenate(hots, axis=1)
        weight = jnp.concatenate(weights, axis=1)
        found = lax.dot_general(weight, hot, (((1,), (1,)), ((), ())), preferred_element_type=jnp.float32)
        found = found[:16] + found[16:32] + found[32:48]
        tables.append(found[:8] + pltpu.roll(found[8:], 1, 1))
    counts = jnp.concatenate(tables, axis=0)
    row = lax.broadcasted_iota(jnp.int32, counts.shape, 0) & 7
    running = counts
    for step in (1, 2, 4):
        running = running + jnp.where(row >= step, pltpu.roll(running, step, 0), 0.0)
    sums = [jnp.broadcast_to(jnp.sum(t, axis=0, keepdims=True), (8, LANES)) for t in tables]
    sums = jnp.concatenate(sums, axis=0)
    upper = (
        lax.broadcasted_iota(jnp.int32, (LANES, LANES), 0) < lax.broadcasted_iota(jnp.int32, (LANES, LANES), 1)
    ).astype(jnp.float32)
    prior = jnp.dot(sums, upper, precision=lax.Precision.HIGHEST, preferred_element_type=jnp.float32)
    earlier = prior + (running - counts)
    share = jnp.clip((0.5 * total - earlier) / jnp.maximum(counts, 1.0), 0.0, 1.0)
    scales = []
    for t in range(groups):
        part = jnp.sum(share[8 * t : 8 * t + 8], axis=0, keepdims=True)
        scales.append(1.4826 * (width * jnp.sum(part, axis=1, keepdims=True)))
    return scales


def exchange_kernel(n, m, moved_ref, score_ref, scale_ref, peak_ref, recv1, scored, send2, recv2, grid, best, bests, send1_sem, recv1_sem, send2_sem, recv2_sem, send3_sem, recv3_sem):
    me, group = lax.axis_index("sta"), lax.axis_index("tpl")
    groups = send2.shape[1]
    chunk = moved_ref.shape[0] // n
    count = chunk // groups
    own = score_ref.shape[0]

    def peer(d):
        return lax.rem(me + d, n)

    def fellow(e):
        return lax.rem(group + e, m)

    barrier = pltpu.get_barrier_semaphore()

    def greet(d, carry):
        pl.semaphore_signal(barrier, inc=1, device_id={"sta": peer(d), "tpl": group}, device_id_type=MESH)
        return carry

    lax.fori_loop(1, n, greet, 0)
    for e in range(1, m):
        pl.semaphore_signal(barrier, inc=1, device_id={"sta": me, "tpl": fellow(e)}, device_id_type=MESH)
    pl.semaphore_wait(barrier, n + m - 2)

    def copy1(d):
        rows = pl.ds(pl.multiple_of(peer(d) * chunk, 8), chunk)
        return pltpu.make_async_remote_copy(
            src_ref=moved_ref.at[rows],
            dst_ref=recv1.at[d],
            send_sem=send1_sem.at[d],
            recv_sem=recv1_sem.at[d],
            device_id={"sta": peer(d), "tpl": group},
            device_id_type=MESH,
        )

    def copy2(d):
        return pltpu.make_async_remote_copy(
            src_ref=send2.at[peer(d)],
            dst_ref=recv2.at[me],
            send_sem=send2_sem.at[d],
            recv_sem=recv2_sem.at[d],
            device_id={"sta": peer(d), "tpl": group},
            device_id_type=MESH,
        )

    def copy3(e):
        return pltpu.make_async_remote_copy(
            src_ref=best,
            dst_ref=bests.at[e],
            send_sem=send3_sem.at[e],
            recv_sem=recv3_sem.at[e],
            device_id={"sta": me, "tpl": fellow(e)},
            device_id_type=MESH,
        )

    def start1(d, carry):
        copy1(d).start()
        return carry

    lax.fori_loop(1, n, start1, 0)

    def gather1(d, acc):
        copy1(d).wait_recv()
        return acc + recv1[d]

    stack = lax.fori_loop(1, n, gather1, moved_ref[pl.ds(pl.multiple_of(me * chunk, 8), chunk), :])
    scales = deviation_scale(stack, groups, n * own)
    scored[chunk:, :] = jnp.zeros((8, LANES), jnp.float32)
    for t in range(groups):
        scored[t * count : (t + 1) * count, :] = stack[t * count : (t + 1) * count, :] / scales[t]
    scale = jnp.concatenate(scales, axis=0)
    lane = lax.broadcasted_iota(jnp.int32, (groups, LANES), 1)
    for j in range(n):
        begin, rest = divmod(own * j, LANES)
        near = scored[pl.ds(begin, groups, stride=count), :]
        if rest:
            after = scored[pl.ds(begin + 1, groups, stride=count), :]
            near = pltpu.roll(jnp.where(lane >= rest, near, after), LANES - rest, 1)
        send2[j] = jnp.where(lane < own, near, scale)

    def start2(d, carry):
        copy2(d).start()
        return carry

    lax.fori_loop(1, n, start2, 0)
    recv2[me] = send2[me]

    def wait2(d, carry):
        copy2(d).wait_recv()
        return carry

    lax.fori_loop(1, n, wait2, 0)
    for i in range(n):
        grid[i * groups : (i + 1) * groups, :] = recv2[i]
    whole = grid[...]
    top = jnp.max(whole, axis=0, keepdims=True)
    best[...] = jnp.broadcast_to(top, best.shape)
    for e in range(1, m):
        copy3(e).start()
    turned = whole.T
    score_ref[...] = turned[:own, :]
    scale_ref[...] = turned[own : own + 1, :]
    for e in range(1, m):
        copy3(e).wait_recv()
        top = jnp.maximum(top, bests[e][:1])
    peak_ref[...] = top[:, :own]

    def finish(d, carry):
        copy1(d).wait_send()
        copy2(d).wait_send()
        return carry

    lax.fori_loop(1, n, finish, 0)
    for e in range(1, m):
        copy3(e).wait_send()


def exchange(moved, rows, n, m):
    chunk = moved.shape[0] // n
    groups = rows // n
    return pl.pallas_call(
        functools.partial(exchange_kernel, n, m),
        out_shape=(
            jax.ShapeDtypeStruct((TOUT_DEV, rows), jnp.float32),
            jax.ShapeDtypeStruct((1, rows), jnp.float32),
            jax.ShapeDtypeStruct((1, TOUT_DEV), jnp.float32),
        ),
        in_specs=[pl.BlockSpec(memory_space=pltpu.VMEM)],
        out_specs=(pl.BlockSpec(memory_space=pltpu.VMEM),) * 3,
        scratch_shapes=[
            pltpu.VMEM((n, chunk, LANES), jnp.float32),
            pltpu.VMEM((chunk + 8, LANES), jnp.float32),
            pltpu.VMEM((n, groups, LANES), jnp.float32),
            pltpu.VMEM((n, groups, LANES), jnp.float32),
            pltpu.VMEM((rows, LANES), jnp.float32),
            pltpu.VMEM((8, LANES), jnp.float32),
            pltpu.VMEM((m, 8, LANES), jnp.float32),
            pltpu.SemaphoreType.DMA((n,)),
            pltpu.SemaphoreType.DMA((n,)),
            pltpu.SemaphoreType.DMA((n,)),
            pltpu.SemaphoreType.DMA((n,)),
            pltpu.SemaphoreType.DMA((m,)),
            pltpu.SemaphoreType.DMA((m,)),
        ],
        compiler_params=pltpu.CompilerParams(collective_id=0, has_side_effects=True),
    )(moved)


def on_device(waveform, templates, lags, present):
    n, m = lax.axis_size("sta"), lax.axis_size("tpl")
    rows = templates.shape[0]
    moved = correlate(waveform[0], templates[:, 0, :], lags[:, 0], present, TOUT_DEV * n)
    score, scale_mad, peak = exchange(moved, rows, n, m)
    return (score, scale_mad[0], peak[0])


def solution(mesh):
    placed = (P("sta", None, None), P("tpl", "sta", None), P("tpl", "sta"), P("tpl", "sta"))
    return jax.shard_map(
        on_device,
        mesh=mesh,
        in_specs=placed,
        out_specs=(P("sta", "tpl"), P("tpl"), P("sta")),
        check_vma=False,
    )
```

```python
import functools

import jax
import jax.numpy as jnp
from jax import lax
from jax.experimental import pallas as pl
from jax.experimental.pallas import tpu as pltpu
from jax.sharding import PartitionSpec as P

LEN = 512
LAG = 3000
BINS = 1024
TOUT_DEV = 48
LANES = 128
MESH = pl.DeviceIdType.MESH


def ceil_to(value, step):
    return -(-value // step) * step


def build_hankel(wave_ref, record, hankel):
    chans, samples = wave_ref.shape
    padded = record.shape[1]
    span = hankel.shape[2]
    record[...] = jnp.zeros_like(record)
    record[:, :samples] = wave_ref[...].astype(jnp.float32)
    row = lax.broadcasted_iota(jnp.int32, (8, padded), 0)
    for c in range(chans):
        base = jnp.broadcast_to(record[c : c + 1, :], (8, padded))
        for bit in (1, 2, 4):
            base = jnp.where((row & bit) != 0, pltpu.roll(base, padded - bit, 1), base)
        for g in range(LANES // 16):
            low = pltpu.roll(base, padded - 16 * g, 1) if g else base
            high = pltpu.roll(base, padded - 16 * g - 8, 1)
            both = jnp.concatenate([low[:, :span], high[:, :span]], axis=0)
            hankel[c, 16 * g : 16 * g + 16, :] = both.astype(jnp.bfloat16)


def correlate_blocks(blocks, stride, pattern_ref, hankel, corr):
    chans = hankel.shape[0]
    rows = pattern_ref.shape[0]
    pattern = pattern_ref[...]
    wide = pattern.astype(jnp.float32)
    factor = 1.0 / jnp.sqrt(jnp.sum(wide * wide, axis=1, keepdims=True) + 1e-06)
    for b in range(blocks):
        parts = []
        for c in range(chans):
            for q in range(LEN // LANES):
                begin = 2 * LANES * b + LANES * q
                parts.append(hankel[c, :, begin : begin + 2 * LANES])
        columns = jnp.concatenate(parts, axis=0)
        result = jnp.dot(pattern, columns, preferred_element_type=jnp.float32) * factor
        corr[pl.ds(2 * b, rows, stride=stride), :] = result[:, :LANES]
        corr[pl.ds(2 * b + 1, rows, stride=stride), :] = result[:, LANES:]


def deviation_scale(stack, groups, total):
    width = 512.0 / BINS
    count = stack.shape[0] // groups
    position = jnp.clip(jnp.abs(stack) / width - 0.5, 0.0, BINS - 1.0)
    lower = jnp.minimum(jnp.floor(position), BINS - 2.0)
    coarse = jnp.floor(lower * 0.125)
    fine = position - 8.0 * coarse
    sub = lax.broadcasted_iota(jnp.int32, (LANES, LANES), 0).astype(jnp.float32)
    few = lax.broadcasted_iota(jnp.int32, (16, LANES), 0).astype(jnp.float32)
    tables = []
    for t in range(groups):
        hots, weights = [], []
        for a in range(count):
            r = t * count + a
            hots.append((coarse[r : r + 1, :] == sub).astype(jnp.float32).astype(jnp.bfloat16))
            hat = jnp.maximum(1.0 - jnp.abs(fine[r : r + 1, :] - few), 0.0)
            first = hat.astype(jnp.bfloat16)
            left = hat - first.astype(jnp.float32)
            second = left.astype(jnp.bfloat16)
            third = (left - second.astype(jnp.float32)).astype(jnp.bfloat16)
            weights.append(jnp.concatenate([first, second, third], axis=0))
        hot = jnp.concatenate(hots, axis=1)
        weight = jnp.concatenate(weights, axis=1)
        found = lax.dot_general(weight, hot, (((1,), (1,)), ((), ())), preferred_element_type=jnp.float32)
        found = found[:16] + found[16:32] + found[32:48]
        tables.append(found[:8] + pltpu.roll(found[8:], 1, 1))
    counts = jnp.concatenate(tables, axis=0)
    row = lax.broadcasted_iota(jnp.int32, counts.shape, 0) & 7
    running = counts
    for step in (1, 2, 4):
        running = running + jnp.where(row >= step, pltpu.roll(running, step, 0), 0.0)
    sums = [jnp.broadcast_to(jnp.sum(t, axis=0, keepdims=True), (8, LANES)) for t in tables]
    sums = jnp.concatenate(sums, axis=0)
    upper = (
        lax.broadcasted_iota(jnp.int32, (LANES, LANES), 0) < lax.broadcasted_iota(jnp.int32, (LANES, LANES), 1)
    ).astype(jnp.float32)
    prior = jnp.dot(sums, upper, precision=lax.Precision.HIGHEST, preferred_element_type=jnp.float32)
    earlier = prior + (running - counts)
    share = jnp.clip((0.5 * total - earlier) / jnp.maximum(counts, 1.0), 0.0, 1.0)
    scales = []
    for t in range(groups):
        part = jnp.sum(share[8 * t : 8 * t + 8], axis=0, keepdims=True)
        scales.append(1.4826 * (width * jnp.sum(part, axis=1, keepdims=True)))
    return scales


def stack_kernel(n, m, own, blocks, stride, lags_ref, present_ref, wave_ref, pattern_ref, out_ref, record, hankel, corr, moved, recv1, scored, send2, recv2, send3, recv3, send1_sem, recv1_sem, send2_sem, recv2_sem, send3_sem, recv3_sem):
    me, group = lax.axis_index("sta"), lax.axis_index("tpl")
    groups = send2.shape[1]
    chunk = moved.shape[1]
    count = chunk // groups
    rows = n * groups

    def peer(d):
        return lax.rem(me + d, n)

    def fellow(e):
        return lax.rem(group + e, m)

    barrier = pltpu.get_barrier_semaphore()
    for e in range(m):

        def greet(d, carry):
            pl.semaphore_signal(barrier, inc=1, device_id={"sta": peer(d), "tpl": fellow(e)}, device_id_type=MESH)
            return carry

        lax.fori_loop(0 if e else 1, n, greet, 0)

    def copy1(d):
        return pltpu.make_async_remote_copy(
            src_ref=moved.at[d],
            dst_ref=recv1.at[d],
            send_sem=send1_sem.at[d],
            recv_sem=recv1_sem.at[d],
            device_id={"sta": peer(d), "tpl": group},
            device_id_type=MESH,
        )

    def copy2(d):
        return pltpu.make_async_remote_copy(
            src_ref=send2.at[peer(d)],
            dst_ref=recv2.at[me],
            send_sem=send2_sem.at[d],
            recv_sem=recv2_sem.at[d],
            device_id={"sta": peer(d), "tpl": group},
            device_id_type=MESH,
        )

    def copy3(e, d):
        return pltpu.make_async_remote_copy(
            src_ref=send3.at[peer(d)],
            dst_ref=recv3.at[e, d],
            send_sem=send3_sem.at[e, d],
            recv_sem=recv3_sem.at[e, d],
            device_id={"sta": peer(d), "tpl": fellow(e)},
            device_id_type=MESH,
        )

    build_hankel(wave_ref, record, hankel)
    correlate_blocks(blocks, stride, pattern_ref, hankel, corr)

    lane = lax.broadcasted_iota(jnp.int32, (count, LANES), 1)

    def shift(d):
        for k in range(groups):
            t = peer(d) * groups + k
            lag = lags_ref[t]
            begin = t * stride + (lag >> 7)
            rest = lag & (LANES - 1)
            near = corr[pl.ds(begin, count), :]
            after = corr[pl.ds(begin + 1, count), :]
            joined = pltpu.roll(jnp.where(lane >= rest, near, after), (LANES - rest) & (LANES - 1), 1)
            moved[d, k * count : (k + 1) * count, :] = joined * present_ref[t].astype(jnp.float32)

    batch = max(n // 4, 1)
    for begin in range(1, n, batch):
        for d in range(begin, min(begin + batch, n)):
            shift(d)
        if begin == 1:
            pl.semaphore_wait(barrier, n * m - 1)
        for d in range(begin, min(begin + batch, n)):
            copy1(d).start()
    shift(0)

    def gather1(d, acc):
        copy1(d).wait_recv()
        return acc + recv1[d]

    stack = lax.fori_loop(1, n, gather1, moved[0])
    scales = deviation_scale(stack, groups, n * own)
    scored[chunk:, :] = jnp.zeros((8, LANES), jnp.float32)
    for t in range(groups):
        scored[t * count : (t + 1) * count, :] = stack[t * count : (t + 1) * count, :] / scales[t]
    scale = jnp.concatenate(scales, axis=0)
    lane = lax.broadcasted_iota(jnp.int32, (groups, LANES), 1)
    for j in range(n):
        begin, rest = divmod(own * j, LANES)
        near = scored[pl.ds(begin, groups, stride=count), :]
        if rest:
            after = scored[pl.ds(begin + 1, groups, stride=count), :]
            near = pltpu.roll(jnp.where(lane >= rest, near, after), LANES - rest, 1)
        send2[j] = jnp.where(lane < own, near, scale)
        send3[j] = jnp.max(near, axis=0, keepdims=True)

    def start2(d, carry):
        copy2(d).start()
        return carry

    lax.fori_loop(1, n, start2, 0)
    for e in range(1, m):

        def start3(d, carry):
            copy3(e, d).start()
            return carry

        lax.fori_loop(0, n, start3, 0)
    recv2[me] = send2[me]

    def wait2(d, carry):
        copy2(d).wait_recv()
        return carry

    lax.fori_loop(1, n, wait2, 0)
    top = recv2[0]
    out_ref[:groups, :] = top
    for i in range(1, n):
        out_ref[i * groups : (i + 1) * groups, :] = recv2[i]
        top = jnp.maximum(top, recv2[i])
    top = jnp.max(top, axis=0, keepdims=True)
    for e in range(1, m):

        def wait3(d, best):
            copy3(e, d).wait_recv()
            return jnp.maximum(best, recv3[e, d])

        top = lax.fori_loop(0, n, wait3, top)
    out_ref[rows:, :] = jnp.broadcast_to(top, (8, LANES))

    def finish(d, carry):
        copy1(d).wait_send()
        copy2(d).wait_send()
        return carry

    lax.fori_loop(1, n, finish, 0)
    for e in range(1, m):

        def finish3(d, carry):
            copy3(e, d).wait_send()
            return carry

        lax.fori_loop(0, n, finish3, 0)


def stack_and_score(wave, pattern, lags, present, n, m):
    chans, samples = wave.shape
    rows = pattern.shape[0]
    total = TOUT_DEV * n
    blocks = -(-(total + LAG) // (2 * LANES))
    span = 2 * LANES * blocks + LEN - LANES
    padded = span + LANES
    count = total // LANES
    stride = max(2 * blocks, LAG // LANES + count + 2) | 1
    groups = rows // n
    chunk = groups * count
    smem, vmem = pl.BlockSpec(memory_space=pltpu.SMEM), pl.BlockSpec(memory_space=pltpu.VMEM)
    return pl.pallas_call(
        functools.partial(stack_kernel, n, m, TOUT_DEV, blocks, stride),
        out_shape=jax.ShapeDtypeStruct((rows + 8, LANES), jnp.float32),
        in_specs=[smem, smem, vmem, vmem],
        out_specs=vmem,
        scratch_shapes=[
            pltpu.VMEM((chans, padded), jnp.float32),
            pltpu.VMEM((chans, LANES, span), jnp.bfloat16),
            pltpu.VMEM((rows * stride, LANES), jnp.float32),
            pltpu.VMEM((n, chunk, LANES), jnp.float32),
            pltpu.VMEM((n, chunk, LANES), jnp.float32),
            pltpu.VMEM((chunk + 8, LANES), jnp.float32),
            pltpu.VMEM((n, groups, LANES), jnp.float32),
            pltpu.VMEM((n, groups, LANES), jnp.float32),
            pltpu.VMEM((n, 1, LANES), jnp.float32),
            pltpu.VMEM((m, n, 1, LANES), jnp.float32),
            pltpu.SemaphoreType.DMA((n,)),
            pltpu.SemaphoreType.DMA((n,)),
            pltpu.SemaphoreType.DMA((n,)),
            pltpu.SemaphoreType.DMA((n,)),
            pltpu.SemaphoreType.DMA((m, n)),
            pltpu.SemaphoreType.DMA((m, n)),
        ],
        compiler_params=pltpu.CompilerParams(collective_id=0, has_side_effects=True),
    )(lags, present, wave, pattern)


def finish_kernel(grid_ref, score_ref, scale_ref, peak_ref):
    own, rows = score_ref.shape
    turned = grid_ref[:rows, :].T
    score_ref[...] = turned[:own, :]
    scale_ref[...] = turned[own, :]
    peak_ref[...] = grid_ref[rows, :own]


def on_device(waveform, templates, lags, present):
    n, m = lax.axis_size("sta"), lax.axis_size("tpl")
    rows = templates.shape[0]
    grid = stack_and_score(waveform[0], templates[:, 0, :], lags[:, 0], present[:, 0], n, m)
    return pl.pallas_call(
        finish_kernel,
        out_shape=(
            jax.ShapeDtypeStruct((TOUT_DEV, rows), jnp.float32),
            jax.ShapeDtypeStruct((rows,), jnp.float32),
            jax.ShapeDtypeStruct((TOUT_DEV,), jnp.float32),
        ),
    )(grid)


def solution(mesh):
    placed = (P("sta", None, None), P("tpl", "sta", None), P("tpl", "sta"), P("tpl", "sta"))
    return jax.shard_map(
        on_device,
        mesh=mesh,
        in_specs=placed,
        out_specs=(P("sta", "tpl"), P("tpl"), P("sta")),
        check_vma=False,
    )
```

```python
import functools

import jax
import jax.numpy as jnp
from jax import lax
from jax.experimental import pallas as pl
from jax.experimental.pallas import tpu as pltpu
from jax.sharding import PartitionSpec as P

LEN = 512
LAG = 3000
BINS = 1024
TOUT_DEV = 48
LANES = 128
MESH = pl.DeviceIdType.MESH


def ceil_to(value, step):
    return -(-value // step) * step


def build_hankel(wave_ref, record, hankel):
    chans, samples = wave_ref.shape
    padded = record.shape[1]
    span = hankel.shape[2]
    record[...] = jnp.zeros_like(record)
    record[:, :samples] = wave_ref[...].astype(jnp.float32)
    piece = span
    for c in range(chans):
        for start in range(0, span, piece):
            size = min(piece, span - start)
            wide = size + LANES
            row = lax.broadcasted_iota(jnp.int32, (8, wide), 0)
            base = jnp.broadcast_to(record[c : c + 1, start : start + wide], (8, wide))
            for bit in (1, 2, 4):
                base = jnp.where((row & bit) != 0, pltpu.roll(base, wide - bit, 1), base)
            for g in range(LANES // 16):
                low = pltpu.roll(base, wide - 16 * g, 1) if g else base
                high = pltpu.roll(base, wide - 16 * g - 8, 1)
                both = jnp.concatenate([low[:, :size], high[:, :size]], axis=0)
                hankel[c, 16 * g : 16 * g + 16, start : start + size] = both.astype(jnp.bfloat16)


def correlate_blocks(blocks, stride, pattern_ref, hankel, corr):
    chans = hankel.shape[0]
    rows = pattern_ref.shape[0]
    pattern = pattern_ref[...]
    wide = pattern.astype(jnp.float32)
    factor = 1.0 / jnp.sqrt(jnp.sum(wide * wide, axis=1, keepdims=True) + 1e-06)
    for b in range(blocks):
        parts = []
        for c in range(chans):
            for q in range(LEN // LANES):
                begin = 2 * LANES * b + LANES * q
                parts.append(hankel[c, :, begin : begin + 2 * LANES])
        columns = jnp.concatenate(parts, axis=0)
        result = jnp.dot(pattern, columns, preferred_element_type=jnp.float32) * factor
        corr[pl.ds(2 * b, rows, stride=stride), :] = result[:, :LANES]
        corr[pl.ds(2 * b + 1, rows, stride=stride), :] = result[:, LANES:]


def deviation_scale(stack, groups, total):
    width = 512.0 / BINS
    count = stack.shape[0] // groups
    position = jnp.clip(jnp.abs(stack) / width - 0.5, 0.0, BINS - 1.0)
    lower = jnp.minimum(jnp.floor(position), BINS - 2.0)
    coarse = jnp.floor(lower * 0.125)
    fine = position - 8.0 * coarse
    sub = lax.broadcasted_iota(jnp.int32, (LANES, LANES), 0).astype(jnp.float32)
    few = lax.broadcasted_iota(jnp.int32, (16, LANES), 0).astype(jnp.float32)
    tables = []
    for t in range(groups):
        hots, weights = [], []
        for a in range(count):
            r = t * count + a
            hots.append((coarse[r : r + 1, :] == sub).astype(jnp.float32).astype(jnp.bfloat16))
            hat = jnp.maximum(1.0 - jnp.abs(fine[r : r + 1, :] - few), 0.0)
            first = hat.astype(jnp.bfloat16)
            left = hat - first.astype(jnp.float32)
            second = left.astype(jnp.bfloat16)
            third = (left - second.astype(jnp.float32)).astype(jnp.bfloat16)
            weights.append(jnp.concatenate([first, second, third], axis=0))
        hot = jnp.concatenate(hots, axis=1)
        weight = jnp.concatenate(weights, axis=1)
        found = lax.dot_general(weight, hot, (((1,), (1,)), ((), ())), preferred_element_type=jnp.float32)
        found = found[:16] + found[16:32] + found[32:48]
        tables.append(found[:8] + pltpu.roll(found[8:], 1, 1))
    counts = jnp.concatenate(tables, axis=0)
    row = lax.broadcasted_iota(jnp.int32, counts.shape, 0) & 7
    running = counts
    for step in (1, 2, 4):
        running = running + jnp.where(row >= step, pltpu.roll(running, step, 0), 0.0)
    sums = [jnp.broadcast_to(jnp.sum(t, axis=0, keepdims=True), (8, LANES)) for t in tables]
    sums = jnp.concatenate(sums, axis=0)
    upper = (
        lax.broadcasted_iota(jnp.int32, (LANES, LANES), 0) < lax.broadcasted_iota(jnp.int32, (LANES, LANES), 1)
    ).astype(jnp.float32)
    prior = jnp.dot(sums, upper, precision=lax.Precision.HIGHEST, preferred_element_type=jnp.float32)
    earlier = prior + (running - counts)
    share = jnp.clip((0.5 * total - earlier) / jnp.maximum(counts, 1.0), 0.0, 1.0)
    scales = []
    for t in range(groups):
        part = jnp.sum(share[8 * t : 8 * t + 8], axis=0, keepdims=True)
        scales.append(1.4826 * (width * jnp.sum(part, axis=1, keepdims=True)))
    return scales


def stack_kernel(n, m, own, blocks, stride, lags_hbm, present_hbm, wave_hbm, pattern_hbm, out_ref, lags_ref, present_ref, wave_ref, pattern_ref, load_sem, record, hankel, corr, moved, recv1, scored, send2, recv2, send3, recv3, send1_sem, recv1_sem, send2_sem, recv2_sem, send3_sem, recv3_sem):
    me, group = lax.axis_index("sta"), lax.axis_index("tpl")
    groups = send2.shape[1]
    chunk = moved.shape[1]
    count = chunk // groups
    rows = n * groups

    def peer(d):
        return lax.rem(me + d, n)

    def fellow(e):
        return lax.rem(group + e, m)

    loads = [
        pltpu.make_async_copy(source, target, load_sem.at[k])
        for k, (source, target) in enumerate(
            ((wave_hbm, wave_ref), (pattern_hbm, pattern_ref), (lags_hbm, lags_ref), (present_hbm, present_ref))
        )
    ]
    for load in loads:
        load.start()

    barrier = pltpu.get_barrier_semaphore()
    for e in range(m):

        def greet(d, carry):
            pl.semaphore_signal(barrier, inc=1, device_id={"sta": peer(d), "tpl": fellow(e)}, device_id_type=MESH)
            return carry

        lax.fori_loop(0 if e else 1, n, greet, 0)

    def copy1(d):
        return pltpu.make_async_remote_copy(
            src_ref=moved.at[d],
            dst_ref=recv1.at[d],
            send_sem=send1_sem.at[d],
            recv_sem=recv1_sem.at[d],
            device_id={"sta": peer(d), "tpl": group},
            device_id_type=MESH,
        )

    def copy2(d):
        return pltpu.make_async_remote_copy(
            src_ref=send2.at[peer(d)],
            dst_ref=recv2.at[me],
            send_sem=send2_sem.at[d],
            recv_sem=recv2_sem.at[d],
            device_id={"sta": peer(d), "tpl": group},
            device_id_type=MESH,
        )

    def copy3(e, d):
        return pltpu.make_async_remote_copy(
            src_ref=send3.at[peer(d)],
            dst_ref=recv3.at[e, d],
            send_sem=send3_sem.at[e, d],
            recv_sem=recv3_sem.at[e, d],
            device_id={"sta": peer(d), "tpl": fellow(e)},
            device_id_type=MESH,
        )

    loads[0].wait()
    build_hankel(wave_ref, record, hankel)
    loads[1].wait()
    correlate_blocks(blocks, stride, pattern_ref, hankel, corr)

    loads[2].wait()
    loads[3].wait()
    lane = lax.broadcasted_iota(jnp.int32, (count, LANES), 1)

    def shift(d):
        for k in range(groups):
            t = peer(d) * groups + k
            lag = lags_ref[t]
            begin = t * stride + (lag >> 7)
            rest = lag & (LANES - 1)
            near = corr[pl.ds(begin, count), :]
            after = corr[pl.ds(begin + 1, count), :]
            joined = pltpu.roll(jnp.where(lane >= rest, near, after), (LANES - rest) & (LANES - 1), 1)
            moved[d, k * count : (k + 1) * count, :] = joined * present_ref[t].astype(jnp.float32)

    far_first = sorted(range(1, n), key=lambda d: abs(d - n // 2))
    batch = max(n // 4, 1)
    for begin in range(0, n - 1, batch):
        for d in far_first[begin : begin + batch]:
            shift(d)
        if begin == 0:
            pl.semaphore_wait(barrier, n * m - 1)
        for d in far_first[begin : begin + batch]:
            copy1(d).start()
    shift(0)

    def gather1(d, acc):
        copy1(d).wait_recv()
        return acc + recv1[d]

    stack = lax.fori_loop(1, n, gather1, moved[0])
    scales = deviation_scale(stack, groups, n * own)
    scored[chunk:, :] = jnp.zeros((8, LANES), jnp.float32)
    for t in range(groups):
        scored[t * count : (t + 1) * count, :] = stack[t * count : (t + 1) * count, :] / scales[t]
    scale = jnp.concatenate(scales, axis=0)
    lane = lax.broadcasted_iota(jnp.int32, (groups, LANES), 1)
    for j in range(n):
        begin, rest = divmod(own * j, LANES)
        near = scored[pl.ds(begin, groups, stride=count), :]
        if rest:
            after = scored[pl.ds(begin + 1, groups, stride=count), :]
            near = pltpu.roll(jnp.where(lane >= rest, near, after), LANES - rest, 1)
        send2[j] = jnp.where(lane < own, near, scale)
        send3[j] = jnp.max(near, axis=0, keepdims=True)

    for e in range(1, m):

        def start3(d, carry):
            copy3(e, d).start()
            return carry

        lax.fori_loop(0, n, start3, 0)
    def start2(d, carry):
        copy2(d).start()
        return carry

    lax.fori_loop(1, n, start2, 0)
    recv2[me] = send2[me]

    def wait2(d, carry):
        copy2(d).wait_recv()
        return carry

    lax.fori_loop(1, n, wait2, 0)
    top = recv2[0]
    out_ref[:groups, :] = top
    for i in range(1, n):
        out_ref[i * groups : (i + 1) * groups, :] = recv2[i]
        top = jnp.maximum(top, recv2[i])
    top = jnp.max(top, axis=0, keepdims=True)
    for e in range(1, m):

        def wait3(d, best):
            copy3(e, d).wait_recv()
            return jnp.maximum(best, recv3[e, d])

        top = lax.fori_loop(0, n, wait3, top)
    lane = lax.broadcasted_iota(jnp.int32, (8, LANES), 1)
    moved_top = jnp.broadcast_to(pltpu.roll(top, LANES // 2, 1), (8, LANES))
    out_ref[:8, :] = jnp.where(lane < LANES // 2, out_ref[:8, :], moved_top)

    def finish(d, carry):
        copy1(d).wait_send()
        copy2(d).wait_send()
        return carry

    lax.fori_loop(1, n, finish, 0)
    for e in range(1, m):

        def finish3(d, carry):
            copy3(e, d).wait_send()
            return carry

        lax.fori_loop(0, n, finish3, 0)


def stack_and_score(wave, pattern, lags, present, n, m):
    chans, samples = wave.shape
    rows = pattern.shape[0]
    total = TOUT_DEV * n
    blocks = -(-(total + LAG) // (2 * LANES))
    span = 2 * LANES * blocks + LEN - LANES
    padded = span + LANES
    count = total // LANES
    stride = max(2 * blocks, LAG // LANES + count + 2) | 1
    groups = rows // n
    chunk = groups * count
    vmem = pl.BlockSpec(memory_space=pltpu.VMEM)
    return pl.pallas_call(
        functools.partial(stack_kernel, n, m, TOUT_DEV, blocks, stride),
        out_shape=jax.ShapeDtypeStruct((rows, LANES), jnp.float32),
        in_specs=[pl.BlockSpec(memory_space=pl.ANY)] * 4,
        out_specs=vmem,
        scratch_shapes=[
            pltpu.SMEM(lags.shape, lags.dtype),
            pltpu.SMEM(present.shape, present.dtype),
            pltpu.VMEM(wave.shape, wave.dtype),
            pltpu.VMEM(pattern.shape, pattern.dtype),
            pltpu.SemaphoreType.DMA((4,)),
            pltpu.VMEM((chans, padded), jnp.float32),
            pltpu.VMEM((chans, LANES, span), jnp.bfloat16),
            pltpu.VMEM((rows * stride, LANES), jnp.float32),
            pltpu.VMEM((n, chunk, LANES), jnp.float32),
            pltpu.VMEM((n, chunk, LANES), jnp.float32),
            pltpu.VMEM((chunk + 8, LANES), jnp.float32),
            pltpu.VMEM((n, groups, LANES), jnp.float32),
            pltpu.VMEM((n, groups, LANES), jnp.float32),
            pltpu.VMEM((n, 1, LANES), jnp.float32),
            pltpu.VMEM((m, n, 1, LANES), jnp.float32),
            pltpu.SemaphoreType.DMA((n,)),
            pltpu.SemaphoreType.DMA((n,)),
            pltpu.SemaphoreType.DMA((n,)),
            pltpu.SemaphoreType.DMA((n,)),
            pltpu.SemaphoreType.DMA((m, n)),
            pltpu.SemaphoreType.DMA((m, n)),
        ],
        compiler_params=pltpu.CompilerParams(collective_id=0, has_side_effects=True),
    )(lags, present, wave, pattern)


def finish_kernel(grid_ref, score_ref, scale_ref, peak_ref):
    own, rows = score_ref.shape
    turned = grid_ref[...].T
    score_ref[...] = turned[:own, :]
    scale_ref[...] = turned[own, :]
    peak_ref[...] = grid_ref[0, LANES // 2 : LANES // 2 + own]


def on_device(waveform, templates, lags, present):
    n, m = lax.axis_size("sta"), lax.axis_size("tpl")
    rows = templates.shape[0]
    grid = stack_and_score(waveform[0], templates[:, 0, :], lags[:, 0], present[:, 0], n, m)
    return pl.pallas_call(
        finish_kernel,
        out_shape=(
            jax.ShapeDtypeStruct((TOUT_DEV, rows), jnp.float32),
            jax.ShapeDtypeStruct((rows,), jnp.float32),
            jax.ShapeDtypeStruct((TOUT_DEV,), jnp.float32),
        ),
    )(grid)


def solution(mesh):
    placed = (P("sta", None, None), P("tpl", "sta", None), P("tpl", "sta"), P("tpl", "sta"))
    return jax.shard_map(
        on_device,
        mesh=mesh,
        in_specs=placed,
        out_specs=(P("sta", "tpl"), P("tpl"), P("sta")),
        check_vma=False,
    )
```
